256 devices in a mesh: row: 8 (over z), col: 32 (over x, y, core).
Axes of the slice: x: 4, y: 4, z: 8, core: 2. Of those that a mesh axis runs over, the one named last changes fastest.
Arguments:
- gradient: bfloat16 [28672, 8192], P('row', 'col'), may hold values from -6 to 6
- projector: bfloat16 [8192, 1024], P('col', 'row'), may hold values from -0.0625 to 0.0625
- first_moment: float32 [1024, 28672], P('col', 'row'), may hold values from -2 to 2
- second_moment: float32 [1024, 28672], P('col', 'row'), may hold values from 0.0001 to 0.01
Outputs:
- update: float32 [28672, 8192], P('row', 'col')
- first_next: float32 [1024, 28672], P('col', 'row')
- second_next: float32 [1024, 28672], P('col', 'row')
The draws below stay inside these ranges and needn't reach their ends.
All inputs are finite; a program needn't handle non-finite values.
Results may differ from the reference program's by a relative error of at most 0.0058.
Values may be sent and summed in bfloat16 or wider, within the bound.
No kernel may reach another device: no remote copies, remote signals or barrier semaphores. Data moves between devices by JAX's collectives and lax.ppermute only.
A program may use at most 64 MiB of HBM per device.

```python
import math
import jax
import jax.numpy as jnp

M = 28672
N = 8192
R = 1024


def levels(key, shape, shards, least, high):
    def one(position, parts):
        heights = jax.random.uniform(jax.random.fold_in(jax.random.fold_in(key, 6), position), (parts,), jnp.float32, least / len(shards), high / len(shards))
        return jnp.repeat(jnp.exp(heights), shape[position] // parts).reshape((-1,) + (1,) * (len(shape) - position - 1))

    loudness = one(*shards[0])
    for cut in shards[1:]:
        loudness = loudness * one(*cut)
    return loudness


def noise(own_key, extent, spread, reach, cuts=(), kind=jnp.bfloat16):
    drawn = spread * jax.random.normal(own_key, extent, jnp.float32)
    if cuts:
        drawn = drawn * levels(own_key, extent, cuts, -0.22, 0.18)
    return jnp.clip(drawn, -reach, reach).astype(kind)


def setup_inputs(seed: int = 0) -> dict:
    arg_keys = jax.random.split(jax.random.key(seed), 5)
    return {
        "gradient": noise(arg_keys[0], (M, N), 1.0, 6.0, ((0, 8), (1, 32))),
        "projector": noise(arg_keys[1], (N, R), N ** -0.5, 0.0625, ((0, 32), (1, 8))),
        "first_moment": noise(arg_keys[2], (R, M), 0.3, 2.0, ((0, 32), (1, 8)), jnp.float32),
        "second_moment": jnp.clip(jnp.exp(math.log(0.01) - 4.6051702 * jax.random.uniform(arg_keys[3], (R, M), jnp.float32) ** levels(arg_keys[3], (R, M), ((0, 32), (1, 8)), -0.2, 0.2)), 0.0001, 0.01),
    }


def reference(gradient, projector, first_moment, second_moment):
    compressed = jnp.dot(projector.T, gradient.T, preferred_element_type=jnp.float32)
    first_next = 0.9 * first_moment + 0.1 * compressed
    second_next = 0.999 * second_moment + 0.001 * compressed * compressed
    corr_first = 1.0 - 0.9 ** 10
    corr_second = 1.0 - 0.999 ** 10
    direction = (first_next / corr_first / (jnp.sqrt(second_next / corr_second) + 1e-08)).astype(jnp.bfloat16)
    update = jnp.dot(direction.T, projector.T, preferred_element_type=jnp.float32)
    return (update, first_next, second_next)
```

```python
import jax
import jax.numpy as jnp
from jax import lax
from jax.experimental import pallas as pl
from jax.experimental.pallas import tpu as pltpu
from jax.sharding import PartitionSpec as P


F32, BF16 = jnp.float32, jnp.bfloat16
SIDE = 4
DEEP = 8
SUB = 64
VMEM = pl.BlockSpec(memory_space=pltpu.VMEM)


def place(x, y, core):
    return (x % SIDE) * 8 + (y % SIDE) * 2 + core


def hop(step, first):
    pairs = []
    for x in range(SIDE):
        for y in range(SIDE):
            for core in range(2):
                along_x = (core == 0) == first
                to = place(x + step, y, core) if along_x else place(x, y + step, core)
                pairs.append((place(x, y, core), to))
    return pairs


def to_core(v):
    return lax.ppermute(v, "col", [(i, i ^ 1) for i in range(32)])


def first_hop(v, step):
    return lax.ppermute(v, "col", hop(step, True))


def second_hop(v, step):
    return lax.ppermute(v, "col", hop(step, False))


def deep_hop(v, step):
    pairs = []
    for z in range(DEEP):
        for i in range(32):
            to = (z + (step if i % 2 == 0 else -step)) % DEEP
            pairs.append((z * 32 + i, to * 32 + i))
    return lax.ppermute(v, ("row", "col"), pairs)


def in_core_order(core, own, other, dim):
    return jnp.where(core == 0, jnp.concatenate([own, other], dim), jnp.concatenate([other, own], dim))


def arrange_kernel(where, own, a1, a2, a3, a4, o1, o2, o34, out):
    z, core, p, q = where[0], where[1], where[2], where[3]
    sign = 1 - 2 * core

    def put(block, h, value):
        sub = block * 2 + h
        x, y = sub // SIDE, sub % SIDE
        r, b = jnp.where(core == 0, x, y), jnp.where(core == 0, y, x)
        out[(r - p + SIDE) % SIDE, (b - q + SIDE) % SIDE] = value

    def put_block(distance, ref, start):
        block = (z + distance + 2 * DEEP) % DEEP
        for h in range(2):
            put(block, h, ref[pl.ds(start + h * SUB, SUB), :])

    put_block(0, own, 0)
    for d, ref in ((1, a1), (2, a2), (3, a3)):
        put_block(-d * sign, ref, 0)
    for d, ref in ((1, o1), (2, o2), (3, o34)):
        put_block(d * sign, ref, 0)
    far = (z + SIDE) % DEEP
    put(far, core, a4[...])
    put(far, 1 - core, o34[pl.ds(2 * SUB, SUB), :])


def arrange(where, *blocks):
    k = blocks[0].shape[1]
    return pl.pallas_call(
        arrange_kernel,
        out_shape=jax.ShapeDtypeStruct((SIDE, SIDE, SUB, k), BF16),
        in_specs=[pl.BlockSpec(memory_space=pltpu.SMEM)] + [VMEM] * len(blocks),
        out_specs=VMEM,
        cost_estimate=pl.CostEstimate(flops=1 << 20, bytes_accessed=1 << 21, transcendentals=0),
        name="arrange",
    )(where, *blocks)


TILE = 448


def update_kernel(where, p_ref, d0, d1, d2, d3, e0, e1, e2, e3, out, w, v):
    step = pl.program_id(0)
    half = pl.num_programs(0) // 2

    @pl.when(step == 0)
    def _():
        columns = pl.ds(pl.multiple_of(where[1] * w.shape[2], w.shape[2]), w.shape[2])
        for a in range(SIDE):
            for b in range(SIDE):
                part = p_ref[a, b, :, columns]
                w[a, b * SUB : (b + 1) * SUB, :] = part
                v[b, a * SUB : (a + 1) * SUB, :] = part

    def product(pieces, weights, start):
        rows = pl.ds(pl.multiple_of(start * TILE, TILE), TILE)
        total = jnp.dot(pieces[0][rows, :], weights[0], preferred_element_type=F32)
        for j in range(1, SIDE):
            total += jnp.dot(pieces[j][rows, :], weights[j], preferred_element_type=F32)
        out[...] = total

    @pl.when(step < half)
    def _():
        product((d0, d1, d2, d3), w, step)

    @pl.when(step >= half)
    def _():
        product((e0, e1, e2, e3), v, step - half)


def back_project(where, ranks, own, other):
    rows = own[0].shape[0]
    k = ranks.shape[3] // 2
    steps = rows // TILE

    def block(step, where):
        core = where[1]
        return jnp.where(step < steps, core * steps + step, (1 - core) * steps + step - steps), 0

    return pl.pallas_call(
        update_kernel,
        out_shape=jax.ShapeDtypeStruct((2 * rows, k), F32),
        grid_spec=pltpu.PrefetchScalarGridSpec(
            num_scalar_prefetch=1,
            grid=(2 * steps,),
            in_specs=[VMEM] * 9,
            out_specs=pl.BlockSpec((TILE, k), block),
            scratch_shapes=[pltpu.VMEM((SIDE, SIDE * SUB, k), BF16)] * 2,
        ),
        compiler_params=pltpu.CompilerParams(dimension_semantics=("arbitrary",)),
        cost_estimate=pl.CostEstimate(flops=2 * 2 * rows * 1024 * k, bytes_accessed=1 << 23, transcendentals=0),
        name="back_project",
    )(where, ranks, *own, *other)


def moments(compressed, first, second):
    return 0.9 * first + 0.1 * compressed, 0.999 * second + 0.001 * compressed * compressed


def direction_of(first_next, second_next):
    corr_first = 1.0 - 0.9**10
    corr_second = 1.0 - 0.999**10
    return (first_next / corr_first / (jnp.sqrt(second_next / corr_second) + 1e-08)).astype(BF16)


def shards(gradient, projector, first_moment, second_moment):
    z = lax.axis_index("row")
    i = lax.axis_index("col")
    core = i % 2
    x, y = i // 8, (i // 2) % SIDE
    where = jnp.stack([z, core, jnp.where(core == 0, x, y), jnp.where(core == 0, y, x)]).astype(jnp.int32)
    rows = gradient.shape[0] // 2

    own = projector.T
    own = in_core_order(core, own, to_core(own), 1)
    a2 = deep_hop(own, 2)
    a1 = deep_hop(own, 1)
    a3 = deep_hop(a2, 1)
    a4 = deep_hop(jnp.where(core == 0, a2[:SUB], a2[SUB:]), 2)
    o1, o2 = to_core(a1), to_core(a2)
    o34 = to_core(jnp.concatenate([a3, a4], 0))

    def half(v, which, dim):
        return lax.dynamic_slice_in_dim(v, which * rows, rows, dim)

    def swapped(v, dim):
        return half(v, core, dim), to_core(half(v, 1 - core, dim))

    grad = in_core_order(core, *swapped(gradient, 0), 1)
    first_part = in_core_order(core, *swapped(first_moment, 1), 0)
    second_part = in_core_order(core, *swapped(second_moment, 1), 0)

    ranks = arrange(where, own, a1, a2, a3, a4, o1, o2, o34)
    partial = lax.dot_general(
        ranks.reshape(1024, -1), grad, (((1,), (1,)), ((), ())), preferred_element_type=F32
    ).astype(BF16)
    partial = partial.reshape(SIDE, 2, 128, rows)

    relay_up = first_hop(partial[2, 0], 1)
    relay_down = first_hop(partial[2, 1], -1)
    from_down_b = first_hop(partial[1, 1], 1)
    from_up_a = first_hop(partial[3, 0], -1)
    from_down_a = first_hop((partial[1, 0].astype(F32) + relay_up.astype(F32)).astype(BF16), 1)
    from_up_b = first_hop((partial[3, 1].astype(F32) + relay_down.astype(F32)).astype(BF16), -1)
    stage = jnp.concatenate(
        [
            partial[0, 0].astype(F32) + from_up_a.astype(F32) + from_down_a.astype(F32),
            partial[0, 1].astype(F32) + from_up_b.astype(F32) + from_down_b.astype(F32),
        ],
        0,
    ).astype(BF16)
    stage = stage.reshape(SIDE, SUB, rows)

    compressed = stage[0].astype(F32)
    for step in (2, 1, 3):
        compressed = compressed + second_hop(stage[step], step).astype(F32)

    direction = direction_of(*moments(compressed, first_part, second_part))
    pieces = {0: direction}
    for step in (2, 1, 3):
        pieces[(SIDE - step) % SIDE] = second_hop(direction, step)
    mine = jnp.concatenate([pieces[j] for j in range(SIDE)], 0).T
    a, b = mine[: rows // 2], mine[rows // 2 :]
    down_a = first_hop(a, 1)
    up_b = first_hop(b, -1)
    down_b = first_hop(b, 1)
    up_a = first_hop(a, -1)
    far_a = first_hop(down_a, 1)
    far_b = first_hop(up_b, -1)
    whole = [
        mine,
        jnp.concatenate([up_a, up_b], 0),
        jnp.concatenate([far_a, far_b], 0),
        jnp.concatenate([down_a, down_b], 0),
    ]
    update = back_project(where, ranks, whole, [to_core(v) for v in whole])

    theirs = to_core(lax.dynamic_slice_in_dim(compressed, (1 - core) * 32, 32, 0))
    kept = lax.dynamic_slice_in_dim(compressed, core * 32, 32, 0)
    first_next, second_next = moments(in_core_order(core, kept, theirs, 1), first_moment, second_moment)
    return update, first_next, second_next


def solution(mesh):
    return jax.shard_map(
        shards,
        mesh=mesh,
        in_specs=(P("row", "col"), P("col", "row"), P("col", "row"), P("col", "row")),
        out_specs=(P("row", "col"), P("col", "row"), P("col", "row")),
        check_vma=False,
    )
```
